32 devices in a mesh: seq: 16 (over z, y, x), tp: 2 (over core).
Axes of the slice: x: 2, y: 2, z: 4, core: 2. Of those that a mesh axis runs over, the one named last changes fastest.
Arguments:
- latent: bfloat16 [2, 16, 256, 1152], P(None, 'seq', 'tp'), may hold values from -6 to 6
- modulation: float32 [2, 9, 1152], replicated, may hold values from -4 to 4
- qkv_spatial: bfloat16 [3, 1152, 1152], P(None, None, 'tp'), may hold values from -0.1875 to 0.1875
- gain_spatial: float32 [2, 72], replicated, may hold values from 0.5 to 1.7
- out_spatial: bfloat16 [1152, 1152], P('tp'), may hold values from -0.1875 to 0.1875
- qkv_temporal: bfloat16 [3, 1152, 1152], P(None, None, 'tp'), may hold values from -0.1875 to 0.1875
- gain_temporal: float32 [2, 72], replicated, may hold values from 0.5 to 1.7
- out_temporal: bfloat16 [1152, 1152], P('tp'), may hold values from -0.1875 to 0.1875
- fc_in: bfloat16 [1152, 4608], P(None, 'tp'), may hold values from -0.1875 to 0.1875
- fc_out: bfloat16 [4608, 1152], P('tp'), may hold values from -0.09375 to 0.09375
Outputs:
- result: bfloat16 [2, 16, 256, 1152], P(None, 'seq', 'tp')
The draws below stay inside these ranges and needn't reach their ends.
All inputs are finite; a program needn't handle non-finite values.
Results may differ from the reference program's by a relative error of at most 0.017.
Values may be sent and summed in bfloat16 or wider, within the bound.
A program may use at most 64 MiB of HBM per device.

```python
import math
import jax
import jax.numpy as jnp
from jax import lax

D = 1152
H = 16
FF = 4608
HD = 72
B = 2
P_SIZE = 256
F = 16
N_TP = 2


def steps_of(rng, extent, split, low, top_value):
    def one(dim, shards_of):
        draws = jax.random.uniform(jax.random.fold_in(jax.random.fold_in(rng, 6), dim), (shards_of,), jnp.float32, low / len(split), top_value / len(split))
        return jnp.repeat(jnp.exp(draws), extent[dim] // shards_of).reshape((-1,) + (1,) * (len(extent) - dim - 1))

    loudness = one(*split[0])
    for cut in split[1:]:
        loudness = loudness * one(*cut)
    return loudness


def bell_draw(key, shape, width, reach, cuts=(), held_as=jnp.bfloat16):
    result = width * jax.random.normal(key, shape, jnp.float32)
    if cuts:
        result = result * steps_of(key, shape, cuts, -0.22, 0.18)
    return jnp.clip(result, -reach, reach).astype(held_as)


def setup_inputs(seed: int = 0) -> dict:
    seeds = jax.random.split(jax.random.key(seed), 11)
    return {
        "latent": bell_draw(seeds[0], (B, F, P_SIZE, D), 1.0, 6.0, ((1, 16), (2, 2))),
        "modulation": bell_draw(seeds[1], (B, 9, D), 0.7, 4.0, (), jnp.float32),
        "qkv_spatial": bell_draw(seeds[2], (3, D, D), D ** -0.5, 0.1875, ((2, 2),)),
        "gain_spatial": jnp.clip(jax.random.uniform(seeds[3], (2, HD), jnp.float32, 0.5, 1.7), 0.5, 1.7),
        "out_spatial": bell_draw(seeds[4], (D, D), D ** -0.5, 0.1875, ((0, 2),)),
        "qkv_temporal": bell_draw(seeds[5], (3, D, D), D ** -0.5, 0.1875, ((2, 2),)),
        "gain_temporal": jnp.clip(jax.random.uniform(seeds[6], (2, HD), jnp.float32, 0.5, 1.7), 0.5, 1.7),
        "out_temporal": bell_draw(seeds[7], (D, D), D ** -0.5, 0.1875, ((0, 2),)),
        "fc_in": bell_draw(seeds[8], (D, FF), D ** -0.5, 0.1875, ((1, 2),)),
        "fc_out": bell_draw(seeds[9], (FF, D), FF ** -0.5, 0.09375, ((0, 2),)),
    }


epsilon = 1e-06

def layer_norm(values):
    average = lax.optimization_barrier(jnp.mean(values, axis=-1, keepdims=True))
    centred = values - average
    variance = lax.optimization_barrier(jnp.mean(centred * centred, axis=-1, keepdims=True))
    return centred * lax.rsqrt(variance + epsilon)

def modulated(field, modulation, offset):
    shift_row = modulation[:, offset][:, None, None, :]
    scale_row = modulation[:, offset + 1][:, None, None, :]
    return (layer_norm(field) * (1.0 + scale_row) + shift_row).astype(jnp.bfloat16)

def project_rows(normed, table, gains, head_dim):
    flat = normed.reshape(-1, normed.shape[-1])
    results = []
    for which_part in range(3):
        projected = jnp.dot(flat, table[which_part], preferred_element_type=jnp.float32)
        if which_part < 2:
            shaped = projected.reshape(projected.shape[0], -1, head_dim)
            shaped = shaped * lax.rsqrt(lax.optimization_barrier(jnp.mean(shaped * shaped, axis=-1, keepdims=True)) + epsilon) * gains[which_part]
            projected = shaped.reshape(projected.shape)
        results.append(projected.astype(jnp.bfloat16).reshape(normed.shape[:-1] + (table.shape[-1],)))
    return results

def attend_one(members, head_dim):
    query_rows, key_rows, value_rows = members
    length, feature_width = query_rows.shape
    head_count = feature_width // head_dim
    query_heads = query_rows.astype(jnp.float32).reshape(length, head_count, head_dim)
    key_heads = key_rows.astype(jnp.float32).reshape(length, head_count, head_dim)
    value_heads = value_rows.astype(jnp.float32).reshape(length, head_count, head_dim)
    scores = jnp.einsum('qhe,khe->hqk', query_heads, key_heads) / math.sqrt(head_dim)
    weights = jnp.exp(scores)
    probabilities = (weights / lax.optimization_barrier(jnp.sum(weights, axis=-1, keepdims=True))).astype(jnp.bfloat16)
    probabilities = lax.optimization_barrier(probabilities).astype(jnp.float32)
    mixed_heads = jnp.einsum('hqk,khe->qhe', probabilities, value_heads)
    return mixed_heads.reshape(length, feature_width).astype(jnp.bfloat16)

def grouped_product(left, right):
    flat = left.reshape(-1, left.shape[-1])
    group_width = flat.shape[1] // N_TP
    total = jnp.zeros((flat.shape[0], right.shape[1]), jnp.float32)
    for group_index in range(N_TP):
        lower = group_index * group_width
        piece_sum = jnp.dot(flat[:, lower:lower + group_width], right[lower:lower + group_width], preferred_element_type=jnp.float32)
        rounded = lax.optimization_barrier(piece_sum.astype(jnp.bfloat16))
        total = total + rounded.astype(jnp.float32)
    return total.astype(jnp.bfloat16).reshape(left.shape[:-1] + (right.shape[1],))

def reference(latent, modulation, qkv_spatial, gain_spatial, out_spatial, qkv_temporal, gain_temporal, out_temporal, fc_in, fc_out):
    head_dim = D // H
    batches, frames, patches, feature_width = latent.shape
    running = latent.astype(jnp.float32)
    normed = modulated(running, modulation, 0)
    query_rows, key_rows, value_rows = project_rows(normed, qkv_spatial, gain_spatial, head_dim)
    grouped = tuple((item.reshape(batches * frames, patches, feature_width) for item in (query_rows, key_rows, value_rows)))
    mixed_heads = lax.map(lambda members: attend_one(members, head_dim), grouped).reshape(batches, frames, patches, feature_width)
    spatial_out = grouped_product(mixed_heads, out_spatial)
    running = running + modulation[:, 2][:, None, None, :] * spatial_out.astype(jnp.float32)
    normed = modulated(running, modulation, 3)
    query_rows, key_rows, value_rows = project_rows(normed, qkv_temporal, gain_temporal, head_dim)
    grouped = tuple((item.transpose(0, 2, 1, 3).reshape(batches * patches, frames, feature_width) for item in (query_rows, key_rows, value_rows)))
    mixed_heads = lax.map(lambda members: attend_one(members, head_dim), grouped)
    mixed_heads = mixed_heads.reshape(batches, patches, frames, feature_width).transpose(0, 2, 1, 3)
    temporal_out = grouped_product(mixed_heads, out_temporal)
    running = running + modulation[:, 5][:, None, None, :] * temporal_out.astype(jnp.float32)
    normed = modulated(running, modulation, 6)
    flat = normed.reshape(-1, feature_width)
    hidden = jax.nn.gelu(jnp.dot(flat, fc_in, preferred_element_type=jnp.float32), approximate=True).astype(jnp.bfloat16)
    mlp_out = grouped_product(hidden, fc_out).reshape(batches, frames, patches, feature_width)
    return (running + modulation[:, 8][:, None, None, :] * mlp_out.astype(jnp.float32)).astype(jnp.bfloat16)
```

```python
import functools
import math

import jax
import jax.numpy as jnp
from jax import lax
from jax.experimental import pallas as pl
from jax.experimental.pallas import tpu as pltpu
from jax.sharding import PartitionSpec as P

MESH = pl.DeviceIdType.MESH
EPSILON = 1e-06
BF16 = jnp.bfloat16
F32 = jnp.float32


def modnorm(rows, mod_ref, b, offset):
    shift = mod_ref[b, offset : offset + 1, :]
    scale = mod_ref[b, offset + 1 : offset + 2, :]
    average = jnp.mean(rows, axis=-1, keepdims=True)
    centred = rows - average
    variance = jnp.mean(centred * centred, axis=-1, keepdims=True)
    return centred * lax.rsqrt(variance + EPSILON) * (1.0 + scale) + shift


def project(rows, table_ref, gain_ref, gain_row, same_head, head_dim):
    results = []
    for part in range(3):
        y = jnp.dot(rows, table_ref[part], preferred_element_type=F32)
        if part < 2:
            squares = jnp.dot((y * y).astype(BF16), same_head, preferred_element_type=F32)
            inverse = lax.rsqrt(squares * (1.0 / head_dim) + EPSILON)
            y = y * inverse * gain_ref[gain_row + part : gain_row + part + 1, :]
        results.append(y.astype(BF16))
    return results


def attend(query, key, value, heads_ref, head_dim, group):
    length, width = query.shape
    factor = math.log2(math.e) / math.sqrt(head_dim)
    if group is not None:
        row = lax.broadcasted_iota(jnp.int32, (length, length), 0)
        column = lax.broadcasted_iota(jnp.int32, (length, length), 1)
        same = lax.rem(row, group) == lax.rem(column, group)
    heads_ref[...] = jnp.zeros_like(heads_ref)
    for head in range(width // head_dim):
        first, last = head * head_dim, (head + 1) * head_dim
        low = first // 128 * 128
        high = min((last + 127) // 128 * 128, width)
        lane = lax.broadcasted_iota(jnp.int32, (1, high - low), 1) + low
        mask = jnp.where((lane >= first) & (lane < last), 1.0, 0.0).astype(BF16)
        scores = lax.dot_general(
            query[:, low:high] * mask,
            key[:, low:high],
            (((1,), (1,)), ((), ())),
            preferred_element_type=F32,
        )
        weights = jnp.exp2(scores * factor)
        if group is not None:
            weights = jnp.where(same, weights, 0.0)
        total = jnp.sum(weights, axis=-1, keepdims=True)
        probabilities = (weights * (1.0 / total)).astype(BF16)
        heads_ref[:, low:high] += jnp.dot(
            probabilities, value[:, low:high] * mask, preferred_element_type=F32
        )
    return heads_ref[...].astype(BF16)


def gelu(u):
    return 0.5 * u * (1.0 + jnp.tanh(math.sqrt(2.0 / math.pi) * (u + 0.044715 * (u * u * u))))


def kernel(
    n,
    head_dim,
    lat,
    mod,
    gains,
    same_head_ref,
    h_qkv_s,
    h_out_s,
    h_qkv_t,
    h_out_t,
    h_in,
    h_out,
    result,
    qkv_s,
    out_s,
    qkv_t,
    out_t,
    w_in,
    w_out,
    lat_peer,
    part,
    got_s,
    running,
    mixed_f32,
    send,
    tokens,
    got_t,
    back_send,
    back,
    normed,
    normed_peer,
    hidden,
    got_m,
    heads,
    w_sem,
    pair_send,
    pair_recv,
    a_send,
    a_recv,
    f_send,
    f_recv,
    b_send,
    b_recv,
    own_sem,
):
    me = lax.axis_index("seq")
    other = 1 - lax.axis_index("tp")
    batches, patches, _ = lat.shape
    block = batches * patches // n
    small = patches // n

    loads = [
        pltpu.make_async_copy(source, target, w_sem.at[i])
        for i, (source, target) in enumerate(
            (
                (h_qkv_s, qkv_s),
                (h_out_s, out_s),
                (h_qkv_t, qkv_t),
                (h_out_t, out_t),
                (h_in, w_in),
                (h_out, w_out),
            )
        )
    ]
    for load in loads:
        load.start()

    barrier = pltpu.get_barrier_semaphore()
    pl.semaphore_signal(barrier, inc=1, device_id={"tp": other}, device_id_type=MESH)
    for k in range(1, n):
        pl.semaphore_signal(
            barrier, inc=1, device_id={"seq": lax.rem(me + k, n)}, device_id_type=MESH
        )
    pl.semaphore_wait(barrier, n)

    def to_peer(source, target, i):
        return pltpu.make_async_remote_copy(
            src_ref=source,
            dst_ref=target,
            send_sem=pair_send.at[i],
            recv_sem=pair_recv.at[i],
            device_id={"tp": other},
            device_id_type=MESH,
        )

    def rows_of(index):
        return pl.ds(pl.multiple_of(index * block, block), block)

    same_head = same_head_ref[...]
    copies = []

    exchange = to_peer(lat, lat_peer, 0)
    exchange.start()
    loads[0].wait()
    exchange.wait()
    loads[1].wait()
    for b in range(batches):
        rows = jnp.concatenate(
            [
                modnorm(lat[b].astype(F32), mod, b, 0).astype(BF16),
                modnorm(lat_peer[b].astype(F32), mod, b, 0).astype(BF16),
            ],
            axis=0,
        )
        query, key, value = project(rows, qkv_s, gains, 0, same_head, head_dim)
        mixed = attend(query, key, value, heads, head_dim, None)
        part[b] = jnp.dot(mixed, out_s[...], preferred_element_type=F32).astype(BF16)
        copy = to_peer(part.at[b, pl.ds(patches, patches)], got_s.at[b], 1 + b)
        copy.start()
        copies.append(copy)
    for b in range(batches):
        copies[b].wait()
        out = (part[b, :patches].astype(F32) + got_s[b].astype(F32)).astype(BF16).astype(F32)
        field = lat[b].astype(F32) + mod[b, 2:3, :] * out
        running[b] = field
        mixed_f32[:, b] = modnorm(field, mod, b, 3).reshape(n, small, field.shape[-1])
    send[...] = mixed_f32[...].reshape(send.shape).astype(BF16)

    def swap(source, target, k, sends, receives):
        to = lax.rem(me + k, n)
        return pltpu.make_async_remote_copy(
            src_ref=source.at[rows_of(to)],
            dst_ref=target.at[rows_of(me)],
            send_sem=sends.at[k],
            recv_sem=receives.at[k],
            device_id={"seq": to},
            device_id_type=MESH,
        )

    def landing(target, k, sends, receives):
        origin = lax.rem(me + n - k, n)
        return pltpu.make_async_remote_copy(
            src_ref=target.at[rows_of(origin)],
            dst_ref=target.at[rows_of(origin)],
            send_sem=sends.at[k],
            recv_sem=receives.at[k],
            device_id={"seq": lax.rem(me + k, n)},
            device_id_type=MESH,
        )

    def forward(origin, k):
        return pltpu.make_async_remote_copy(
            src_ref=tokens.at[0, rows_of(origin)],
            dst_ref=tokens.at[1, rows_of(origin)],
            send_sem=f_send.at[k],
            recv_sem=f_recv.at[k],
            device_id={"tp": other},
            device_id_type=MESH,
        )

    outgoing = [swap(send, tokens.at[0], k, a_send, a_recv) for k in range(1, n)]
    for copy in outgoing:
        copy.start()
    own = pltpu.make_async_copy(send.at[rows_of(me)], tokens.at[0, rows_of(me)], own_sem.at[0])
    own.start()
    own.wait()
    forwards = [forward(me, 0)]
    forwards[0].start()
    for k in range(1, n):
        landing(tokens.at[0], k, a_send, a_recv).wait_recv()
        copy = forward(lax.rem(me + n - k, n), k)
        copy.start()
        forwards.append(copy)
    loads[2].wait()
    loads[3].wait()
    for copy in forwards:
        copy.wait()
    for copy in outgoing:
        copy.wait_send()

    for chunk in (1, 0):
        query, key, value = project(tokens[chunk], qkv_t, gains, 2, same_head, head_dim)
        mixed = attend(query, key, value, heads, head_dim, block)
        part[chunk] = jnp.dot(mixed, out_t[...], preferred_element_type=F32).astype(BF16)
        if chunk == 1:
            share = to_peer(part.at[1], got_t, 1 + batches)
            share.start()
    share.wait()
    back_send[...] = (part[0].astype(F32) + got_t[...].astype(F32)).astype(BF16)

    outgoing = [swap(back_send, back, k, b_send, b_recv) for k in range(1, n)]
    for copy in outgoing:
        copy.start()
    own = pltpu.make_async_copy(back_send.at[rows_of(me)], back.at[rows_of(me)], own_sem.at[1])
    own.start()
    own.wait()
    for k in range(1, n):
        landing(back, k, b_send, b_recv).wait_recv()
    for copy in outgoing:
        copy.wait_send()

    mixed_f32[...] = back[...].astype(F32).reshape(mixed_f32.shape)
    for b in range(batches):
        field = running[b] + mod[b, 5:6, :] * mixed_f32[:, b].reshape(running.shape[1:])
        running[b] = field
        normed[pl.ds(b * patches, patches)] = modnorm(field, mod, b, 6).astype(BF16)
    exchange = to_peer(normed, normed_peer, 2 + batches)
    exchange.start()
    loads[4].wait()
    units = w_in.shape[1]
    tile = next(t for t in (768, 512, 384, 256, 128, units) if units % t == 0)

    def enter(rows, slot):
        for first in range(0, units, tile):
            u = jnp.dot(rows, w_in[:, first : first + tile], preferred_element_type=F32)
            hidden[slot, :, first : first + tile] = gelu(u).astype(BF16)

    enter(normed[...], 0)
    exchange.wait()
    enter(normed_peer[...], 1)
    loads[5].wait()
    part[1] = jnp.dot(hidden[1], w_out[...], preferred_element_type=F32).astype(BF16)
    share = to_peer(part.at[1], got_m, 3 + batches)
    share.start()
    part[0] = jnp.dot(hidden[0], w_out[...], preferred_element_type=F32).astype(BF16)
    share.wait()
    for b in range(batches):
        rows = pl.ds(b * patches, patches)
        out = (part[0, rows].astype(F32) + got_m[rows].astype(F32)).astype(BF16).astype(F32)
        result[b] = (running[b] + mod[b, 8:9, :] * out).astype(BF16)


def layer_norm(values):
    average = jnp.mean(values, axis=-1, keepdims=True)
    centred = values - average
    variance = jnp.mean(centred * centred, axis=-1, keepdims=True)
    return centred * lax.rsqrt(variance + EPSILON)


def modulated(field, modulation, offset):
    shift_row = modulation[:, offset][:, None, None, :]
    scale_row = modulation[:, offset + 1][:, None, None, :]
    return (layer_norm(field) * (1.0 + scale_row) + shift_row).astype(jnp.bfloat16)


def project_heads_any(rows_piece, table, gains, head_dim):
    results = []
    for which_part in range(3):
        projected = jnp.einsum(
            "bfpd,de->bfpe", rows_piece, table[which_part], preferred_element_type=jnp.float32
        )
        if which_part < 2:
            shaped = projected.reshape(
                projected.shape[:-1] + (projected.shape[-1] // head_dim, head_dim)
            )
            shaped = (
                shaped
                * lax.rsqrt(jnp.mean(shaped * shaped, axis=-1, keepdims=True) + EPSILON)
                * gains[which_part]
            )
            projected = shaped.reshape(projected.shape)
        results.append(projected.astype(jnp.bfloat16))
    return jnp.stack(results)


def attend_any(query_rows, key_rows, value_rows, head_dim):
    groups, length, feature_width = query_rows.shape
    head_count = feature_width // head_dim
    query_heads = query_rows.reshape(groups, length, head_count, head_dim)
    key_heads = key_rows.reshape(groups, length, head_count, head_dim)
    value_heads = value_rows.reshape(groups, length, head_count, head_dim)
    block_rows = min(length, 512)

    def one_block(first_row):
        query_block = lax.dynamic_slice_in_dim(query_heads, first_row, block_rows, 1)
        scores = jnp.einsum(
            "gqhe,gkhe->ghqk", query_block, key_heads, preferred_element_type=jnp.float32
        ) / math.sqrt(head_dim)
        weights = jnp.exp(scores)
        probabilities = (weights / jnp.sum(weights, axis=-1, keepdims=True)).astype(jnp.bfloat16)
        return jnp.einsum(
            "ghqk,gkhe->gqhe", probabilities, value_heads, preferred_element_type=jnp.float32
        ).astype(jnp.bfloat16)

    starts = jnp.arange(length // block_rows, dtype=jnp.int32) * block_rows
    pieces = lax.map(one_block, starts)
    return pieces.transpose(1, 0, 2, 3, 4).reshape(groups, length, feature_width)


def frame_attention(query_rows, key_rows, value_rows, head_dim):
    batches, frames, patches, feature_width = query_rows.shape
    members = [
        item.transpose(0, 2, 1, 3).reshape(batches * patches, frames, feature_width)
        for item in (query_rows, key_rows, value_rows)
    ]
    mixed_heads = attend_any(members[0], members[1], members[2], head_dim)
    return mixed_heads.reshape(batches, patches, frames, feature_width).transpose(0, 2, 1, 3)


def body_any_width(
    latent,
    modulation,
    qkv_spatial,
    gain_spatial,
    out_spatial,
    qkv_temporal,
    gain_temporal,
    out_temporal,
    fc_in,
    fc_out,
):
    head_dim = gain_spatial.shape[-1]
    running = latent.astype(jnp.float32)
    normed = modulated(running, modulation, 0)
    packed = project_heads_any(
        lax.all_gather(normed, "tp", axis=2, tiled=True), qkv_spatial, gain_spatial, head_dim
    )
    batches, frames, patches, local_width = packed.shape[1:]
    mixed_heads = attend_any(
        packed[0].reshape(batches * frames, patches, local_width),
        packed[1].reshape(batches * frames, patches, local_width),
        packed[2].reshape(batches * frames, patches, local_width),
        head_dim,
    )
    mixed_heads = mixed_heads.reshape(batches, frames, patches, local_width)
    partial_value = jnp.einsum(
        "bfpe,ed->bfpd", mixed_heads, out_spatial, preferred_element_type=jnp.float32
    )
    spatial_out = lax.psum_scatter(
        partial_value.astype(jnp.bfloat16), "tp", scatter_dimension=2, tiled=True
    )
    running = running + modulation[:, 2][:, None, None, :] * spatial_out.astype(jnp.float32)
    normed = modulated(running, modulation, 3)
    moved_rows = lax.all_to_all(normed, "seq", split_axis=2, concat_axis=1, tiled=True)
    packed = project_heads_any(
        lax.all_gather(moved_rows, "tp", axis=2, tiled=True), qkv_temporal, gain_temporal, head_dim
    )
    mixed_heads = frame_attention(packed[0], packed[1], packed[2], head_dim)
    partial_value = jnp.einsum(
        "bfpe,ed->bfpd", mixed_heads, out_temporal, preferred_element_type=jnp.float32
    )
    shares = lax.psum_scatter(
        partial_value.astype(jnp.bfloat16), "tp", scatter_dimension=2, tiled=True
    )
    temporal_out = lax.all_to_all(shares, "seq", split_axis=1, concat_axis=2, tiled=True)
    running = running + modulation[:, 5][:, None, None, :] * temporal_out.astype(jnp.float32)
    normed = modulated(running, modulation, 6)
    projected = jnp.einsum(
        "bfpd,de->bfpe",
        lax.all_gather(normed, "tp", axis=2, tiled=True),
        fc_in,
        preferred_element_type=jnp.float32,
    )
    hidden = jax.nn.gelu(projected, approximate=True).astype(jnp.bfloat16)
    partial_value = jnp.einsum("bfpe,ed->bfpd", hidden, fc_out, preferred_element_type=jnp.float32)
    mlp_out = lax.psum_scatter(
        partial_value.astype(jnp.bfloat16), "tp", scatter_dimension=2, tiled=True
    )
    return (running + modulation[:, 8][:, None, None, :] * mlp_out.astype(jnp.float32)).astype(
        jnp.bfloat16
    )


def body(n, latent, modulation, qkv_s, gain_s, out_s, qkv_t, gain_t, out_t, fc_in, fc_out):
    batches, frames, patches, width = latent.shape
    head_dim = gain_s.shape[-1]
    local = qkv_s.shape[-1]
    count = batches * patches
    small = patches // n
    lane = jnp.arange(local) // head_dim
    same_head = (lane[:, None] == lane[None, :]).astype(BF16)
    gains = jnp.tile(jnp.concatenate([gain_s, gain_t], axis=0), (1, local // head_dim))
    vmem = pl.BlockSpec(memory_space=pltpu.VMEM)
    hbm = pl.BlockSpec(memory_space=pl.ANY)
    dma = pltpu.SemaphoreType.DMA
    weights = (qkv_s, out_s, qkv_t, out_t, fc_in, fc_out)
    half = (batches, patches, width)
    flat = (count, width)
    out = pl.pallas_call(
        functools.partial(kernel, n, head_dim),
        out_shape=jax.ShapeDtypeStruct(half, BF16),
        in_specs=[vmem] * 4 + [hbm] * 6,
        out_specs=vmem,
        scratch_shapes=[pltpu.VMEM(w.shape, w.dtype) for w in weights]
        + [
            pltpu.VMEM(half, BF16),
            pltpu.VMEM((2, 2 * patches, width), BF16),
            pltpu.VMEM(half, BF16),
            pltpu.VMEM(half, F32),
            pltpu.VMEM((n, batches, small, width), F32),
            pltpu.VMEM(flat, BF16),
            pltpu.VMEM((2,) + flat, BF16),
            pltpu.VMEM(flat, BF16),
            pltpu.VMEM(flat, BF16),
            pltpu.VMEM(flat, BF16),
            pltpu.VMEM(flat, BF16),
            pltpu.VMEM(flat, BF16),
            pltpu.VMEM((2, count, fc_in.shape[1]), BF16),
            pltpu.VMEM(flat, BF16),
            pltpu.VMEM((count, local), F32),
            dma((6,)),
            dma((4 + batches,)),
            dma((4 + batches,)),
            dma((n,)),
            dma((n,)),
            dma((n,)),
            dma((n,)),
            dma((n,)),
            dma((n,)),
            dma((2,)),
        ],
        compiler_params=pltpu.CompilerParams(
            collective_id=0, has_side_effects=True, vmem_limit_bytes=62 * 1024 * 1024
        ),
    )(latent.reshape(half), modulation, gains, same_head, *weights)
    return out.reshape(latent.shape)


def solution(mesh):
    n = mesh.shape["seq"]
    placed = (
        P(None, "seq", "tp", None),
        P(),
        P(None, None, "tp"),
        P(),
        P("tp", None),
        P(None, None, "tp"),
        P(),
        P("tp", None),
        P(None, "tp"),
        P("tp", None),
    )
    return jax.shard_map(
        functools.partial(body, n) if mesh.shape["tp"] == 2 else body_any_width,
        mesh=mesh,
        in_specs=placed,
        out_specs=P(None, "seq", "tp", None),
        check_vma=False,
    )
```

```python
import functools
import math

import jax
import jax.numpy as jnp
from jax import lax
from jax.experimental import pallas as pl
from jax.experimental.pallas import tpu as pltpu
from jax.sharding import PartitionSpec as P

MESH = pl.DeviceIdType.MESH
EPSILON = 1e-06
BF16 = jnp.bfloat16
F32 = jnp.float32


def modnorm(rows, mod_ref, b, offset):
    shift = mod_ref[offset, b : b + 1, :]
    scale = mod_ref[offset + 1, b : b + 1, :]
    average = jnp.mean(rows, axis=-1, keepdims=True)
    centred = rows - average
    variance = jnp.mean(centred * centred, axis=-1, keepdims=True)
    return centred * lax.rsqrt(variance + EPSILON) * (1.0 + scale) + shift


def project(rows, table_ref, gains, same_head, head_dim):
    results = []
    for part in range(3):
        y = lax.dot_general(
            rows, table_ref[part], (((1,), (1,)), ((), ())), preferred_element_type=F32
        )
        if part < 2:
            squares = jnp.dot((y * y).astype(BF16), same_head, preferred_element_type=F32)
            inverse = lax.rsqrt(squares * (1.0 / head_dim) + EPSILON)
            y = y * inverse * gains[part : part + 1, :]
        results.append(y.astype(BF16))
    return results


def attend(query, key, value, heads_ref, head_dim, group):
    length, width = query.shape
    factor = math.log2(math.e) / math.sqrt(head_dim)
    if group is not None:
        row = lax.broadcasted_iota(jnp.int32, (length, length), 0)
        column = lax.broadcasted_iota(jnp.int32, (length, length), 1)
        same = (lax.rem(row, group) == lax.rem(column, group)) & (
            (row < length // 2) == (column < length // 2)
        )
    heads_ref[...] = jnp.zeros_like(heads_ref)
    for head in range(width // head_dim):
        first, last = head * head_dim, (head + 1) * head_dim
        low = first // 128 * 128
        high = min((last + 127) // 128 * 128, width)
        lane = lax.broadcasted_iota(jnp.int32, (1, high - low), 1) + low
        mask = jnp.where((lane >= first) & (lane < last), 1.0, 0.0).astype(BF16)
        scores = lax.dot_general(
            query[:, low:high] * mask,
            key[:, low:high],
            (((1,), (1,)), ((), ())),
            preferred_element_type=F32,
        )
        weights = jnp.exp2(scores * factor)
        if group is not None:
            weights = jnp.where(same, weights, 0.0)
        total = jnp.sum(weights, axis=-1, keepdims=True)
        probabilities = (weights * (1.0 / total)).astype(BF16)
        heads_ref[:, low:high] += jnp.dot(
            probabilities, value[:, low:high] * mask, preferred_element_type=F32
        )
    return heads_ref[...].astype(BF16)


def gelu(u):
    return 0.5 * u * (1.0 + jnp.tanh(math.sqrt(2.0 / math.pi) * (u + 0.044715 * (u * u * u))))


def spread(gain_ref, width):
    head_dim = gain_ref.shape[-1]
    row = lax.broadcasted_iota(jnp.int32, (head_dim, width), 0)
    column = lax.broadcasted_iota(jnp.int32, (head_dim, width), 1)
    place = jnp.where(lax.rem(column, head_dim) == row, 1.0, 0.0)
    return jnp.dot(
        gain_ref[...], place, preferred_element_type=F32, precision=lax.Precision.HIGHEST
    )


def kernel(
    n,
    lat,
    mod,
    gain_s,
    gain_t,
    h_qkv_s,
    h_out_s,
    h_qkv_t,
    h_out_t,
    h_in,
    h_out,
    result,
    qkv_s,
    out_s,
    qkv_t,
    out_t,
    w_in,
    w_out,
    lat_peer,
    part,
    got_s,
    got_t,
    got_m,
    running,
    send,
    tokens,
    back_send,
    back,
    normed,
    normed_peer,
    hidden,
    heads,
    w_sem,
    pair_send,
    pair_recv,
    a_send,
    a_recv,
    f_send,
    f_recv,
    b_send,
    b_recv,
    own_sem,
):
    me = lax.axis_index("seq")
    other = 1 - lax.axis_index("tp")
    batches, patches, depth = lat.shape
    small = patches // n
    head_dim = gain_s.shape[-1]
    width = out_s.shape[0]

    loads = [
        pltpu.make_async_copy(source, target, w_sem.at[i])
        for i, (source, target) in enumerate(
            (
                (h_qkv_s, qkv_s),
                (h_out_s, out_s),
                (h_qkv_t, qkv_t),
                (h_out_t, out_t),
                (h_in, w_in),
                (h_out, w_out),
            )
        )
    ]
    loads[0].start()

    barrier = pltpu.get_barrier_semaphore()
    pl.semaphore_signal(barrier, inc=1, device_id={"tp": other}, device_id_type=MESH)
    for k in range(1, n):
        pl.semaphore_signal(
            barrier, inc=1, device_id={"seq": lax.rem(me + k, n)}, device_id_type=MESH
        )
    row_head = lax.div(lax.broadcasted_iota(jnp.int32, (width, 1), 0), head_dim)
    column_head = lax.div(lax.broadcasted_iota(jnp.int32, (1, width), 1), head_dim)
    same_head = jnp.where(row_head == column_head, 1.0, 0.0).astype(BF16)
    gains_s = spread(gain_s, width)
    gains_t = spread(gain_t, width)
    pl.semaphore_wait(barrier, n)

    def to_peer(source, target, i):
        return pltpu.make_async_remote_copy(
            src_ref=source,
            dst_ref=target,
            send_sem=pair_send.at[i],
            recv_sem=pair_recv.at[i],
            device_id={"tp": other},
            device_id_type=MESH,
        )

    def swap(source, target, b, k, sends, receives):
        to = lax.rem(me + k, n)
        return pltpu.make_async_remote_copy(
            src_ref=source.at[to, b],
            dst_ref=target.at[me, b],
            send_sem=sends.at[b * n + k],
            recv_sem=receives.at[b * n + k],
            device_id={"seq": to},
            device_id_type=MESH,
        )

    def landing(target, b, k, sends, receives):
        origin = lax.rem(me + n - k, n)
        return pltpu.make_async_remote_copy(
            src_ref=target.at[origin, b],
            dst_ref=target.at[origin, b],
            send_sem=sends.at[b * n + k],
            recv_sem=receives.at[b * n + k],
            device_id={"seq": lax.rem(me + k, n)},
            device_id_type=MESH,
        )

    def forward(source, origin, b, k):
        return pltpu.make_async_remote_copy(
            src_ref=source,
            dst_ref=tokens.at[1, origin, b],
            send_sem=f_send.at[b * n + k],
            recv_sem=f_recv.at[b * n + k],
            device_id={"tp": other},
            device_id_type=MESH,
        )

    outgoing = []

    exchange = to_peer(lat, lat_peer, 0)
    exchange.start()
    loads[0].wait()
    for load in loads[1:]:
        load.start()
    exchange.wait()
    shares = []
    owns = []
    forwards = []

    def leave(b):
        shares[b].wait()
        out = (part[b, :patches].astype(F32) + got_s[b].astype(F32)).astype(BF16).astype(F32)
        field = lat[b].astype(F32) + mod[2, b : b + 1, :] * out
        running[b] = field
        send[:, b] = modnorm(field, mod, b, 3).reshape(n, small, depth).astype(BF16)
        for k in range(1, n):
            copy = swap(send, tokens.at[0], b, k, a_send, a_recv)
            copy.start()
            outgoing.append(copy)
        own = pltpu.make_async_copy(send.at[me, b], tokens.at[0, me, b], own_sem.at[b])
        own.start()
        owns.append(own)
        copy = forward(send.at[me, b], me, b, 0)
        copy.start()
        forwards.append([copy])

    for b in range(batches):
        rows = jnp.concatenate(
            [
                modnorm(lat[b].astype(F32), mod, b, 0).astype(BF16),
                modnorm(lat_peer[b].astype(F32), mod, b, 0).astype(BF16),
            ],
            axis=0,
        )
        query, key, value = project(rows, qkv_s, gains_s, same_head, head_dim)
        if b > 0:
            leave(b - 1)
        else:
            loads[1].wait()
        mixed = attend(query, key, value, heads, head_dim, None)
        part[b] = jnp.dot(mixed, out_s[...], preferred_element_type=F32).astype(BF16)
        copy = to_peer(part.at[b, pl.ds(patches, patches)], got_s.at[b], 1 + b)
        copy.start()
        shares.append(copy)
    leave(batches - 1)

    loads[2].wait()
    loads[3].wait()
    returns = []

    def give_back(b):
        returns[b].wait()
        out = (part[b, :patches].astype(F32) + got_t[b].astype(F32)).astype(BF16)
        back_send[:, b] = out.astype(F32).reshape(n, small, depth).astype(BF16)
        for k in range(1, n):
            copy = swap(back_send, back, b, k, b_send, b_recv)
            copy.start()
            outgoing.append(copy)
        own = pltpu.make_async_copy(back_send.at[me, b], back.at[me, b], own_sem.at[batches + b])
        own.start()
        owns.append(own)

    for b in range(batches):
        if b > 0:
            give_back(b - 1)
        for k in range(1, n):
            landing(tokens.at[0], b, k, a_send, a_recv).wait_recv()
            origin = lax.rem(me + n - k, n)
            copy = forward(tokens.at[0, origin, b], origin, b, k)
            copy.start()
            forwards[b].append(copy)
        owns[b].wait()
        for copy in forwards[b]:
            copy.wait()
        rows = jnp.concatenate(
            [tokens[i, :, b].astype(F32).reshape(patches, depth) for i in range(2)], axis=0
        ).astype(BF16)
        query, key, value = project(rows, qkv_t, gains_t, same_head, head_dim)
        mixed = attend(query, key, value, heads, head_dim, small)
        part[b] = jnp.dot(mixed, out_t[...], preferred_element_type=F32).astype(BF16)
        copy = to_peer(part.at[b, pl.ds(patches, patches)], got_t.at[b], 1 + batches + b)
        copy.start()
        returns.append(copy)
    give_back(batches - 1)

    loads[4].wait()
    loads[5].wait()
    units = w_in.shape[1]
    tile = next(t for t in (768, 512, 384, 256, 128, units) if units % t == 0)
    ends = []
    for b in range(batches):
        for k in range(1, n):
            landing(back, b, k, b_send, b_recv).wait_recv()
        owns[batches + b].wait()
        field = running[b] + mod[5, b : b + 1, :] * back[:, b].astype(F32).reshape(patches, depth)
        running[b] = field
        normed[b] = modnorm(field, mod, b, 6).astype(BF16)
        exchange = to_peer(normed.at[b], normed_peer.at[b], 1 + 2 * batches + b)
        exchange.start()
        exchange.wait()
        rows = jnp.concatenate([normed[b], normed_peer[b]], axis=0)
        for first in range(0, units, tile):
            u = jnp.dot(rows, w_in[:, first : first + tile], preferred_element_type=F32)
            hidden[:, first : first + tile] = gelu(u).astype(BF16)
        part[b] = jnp.dot(hidden[...], w_out[...], preferred_element_type=F32).astype(BF16)
        copy = to_peer(part.at[b, pl.ds(patches, patches)], got_m.at[b], 1 + 3 * batches + b)
        copy.start()
        ends.append(copy)
    for copy in outgoing:
        copy.wait_send()
    for b in range(batches):
        ends[b].wait()
        out = (part[b, :patches].astype(F32) + got_m[b].astype(F32)).astype(BF16).astype(F32)
        result[b] = (running[b] + mod[8, b : b + 1, :] * out).astype(BF16)


def layer_norm(values):
    average = jnp.mean(values, axis=-1, keepdims=True)
    centred = values - average
    variance = jnp.mean(centred * centred, axis=-1, keepdims=True)
    return centred * lax.rsqrt(variance + EPSILON)


def modulated(field, modulation, offset):
    shift_row = modulation[:, offset][:, None, None, :]
    scale_row = modulation[:, offset + 1][:, None, None, :]
    return (layer_norm(field) * (1.0 + scale_row) + shift_row).astype(jnp.bfloat16)


def project_heads_any(rows_piece, table, gains, head_dim):
    results = []
    for which_part in range(3):
        projected = jnp.einsum(
            "bfpd,de->bfpe", rows_piece, table[which_part], preferred_element_type=jnp.float32
        )
        if which_part < 2:
            shaped = projected.reshape(
                projected.shape[:-1] + (projected.shape[-1] // head_dim, head_dim)
            )
            shaped = (
                shaped
                * lax.rsqrt(jnp.mean(shaped * shaped, axis=-1, keepdims=True) + EPSILON)
                * gains[which_part]
            )
            projected = shaped.reshape(projected.shape)
        results.append(projected.astype(jnp.bfloat16))
    return jnp.stack(results)


def attend_any(query_rows, key_rows, value_rows, head_dim):
    groups, length, feature_width = query_rows.shape
    head_count = feature_width // head_dim
    query_heads = query_rows.reshape(groups, length, head_count, head_dim)
    key_heads = key_rows.reshape(groups, length, head_count, head_dim)
    value_heads = value_rows.reshape(groups, length, head_count, head_dim)
    block_rows = min(length, 512)

    def one_block(first_row):
        query_block = lax.dynamic_slice_in_dim(query_heads, first_row, block_rows, 1)
        scores = jnp.einsum(
            "gqhe,gkhe->ghqk", query_block, key_heads, preferred_element_type=jnp.float32
        ) / math.sqrt(head_dim)
        weights = jnp.exp(scores)
        probabilities = (weights / jnp.sum(weights, axis=-1, keepdims=True)).astype(jnp.bfloat16)
        return jnp.einsum(
            "ghqk,gkhe->gqhe", probabilities, value_heads, preferred_element_type=jnp.float32
        ).astype(jnp.bfloat16)

    starts = jnp.arange(length // block_rows, dtype=jnp.int32) * block_rows
    pieces = lax.map(one_block, starts)
    return pieces.transpose(1, 0, 2, 3, 4).reshape(groups, length, feature_width)


def frame_attention(query_rows, key_rows, value_rows, head_dim):
    batches, frames, patches, feature_width = query_rows.shape
    members = [
        item.transpose(0, 2, 1, 3).reshape(batches * patches, frames, feature_width)
        for item in (query_rows, key_rows, value_rows)
    ]
    mixed_heads = attend_any(members[0], members[1], members[2], head_dim)
    return mixed_heads.reshape(batches, patches, frames, feature_width).transpose(0, 2, 1, 3)


def body_any_width(
    latent,
    modulation,
    qkv_spatial,
    gain_spatial,
    out_spatial,
    qkv_temporal,
    gain_temporal,
    out_temporal,
    fc_in,
    fc_out,
):
    head_dim = gain_spatial.shape[-1]
    running = latent.astype(jnp.float32)
    normed = modulated(running, modulation, 0)
    packed = project_heads_any(
        lax.all_gather(normed, "tp", axis=2, tiled=True), qkv_spatial, gain_spatial, head_dim
    )
    batches, frames, patches, local_width = packed.shape[1:]
    mixed_heads = attend_any(
        packed[0].reshape(batches * frames, patches, local_width),
        packed[1].reshape(batches * frames, patches, local_width),
        packed[2].reshape(batches * frames, patches, local_width),
        head_dim,
    )
    mixed_heads = mixed_heads.reshape(batches, frames, patches, local_width)
    partial_value = jnp.einsum(
        "bfpe,ed->bfpd", mixed_heads, out_spatial, preferred_element_type=jnp.float32
    )
    spatial_out = lax.psum_scatter(
        partial_value.astype(jnp.bfloat16), "tp", scatter_dimension=2, tiled=True
    )
    running = running + modulation[:, 2][:, None, None, :] * spatial_out.astype(jnp.float32)
    normed = modulated(running, modulation, 3)
    moved_rows = lax.all_to_all(normed, "seq", split_axis=2, concat_axis=1, tiled=True)
    packed = project_heads_any(
        lax.all_gather(moved_rows, "tp", axis=2, tiled=True), qkv_temporal, gain_temporal, head_dim
    )
    mixed_heads = frame_attention(packed[0], packed[1], packed[2], head_dim)
    partial_value = jnp.einsum(
        "bfpe,ed->bfpd", mixed_heads, out_temporal, preferred_element_type=jnp.float32
    )
    shares = lax.psum_scatter(
        partial_value.astype(jnp.bfloat16), "tp", scatter_dimension=2, tiled=True
    )
    temporal_out = lax.all_to_all(shares, "seq", split_axis=1, concat_axis=2, tiled=True)
    running = running + modulation[:, 5][:, None, None, :] * temporal_out.astype(jnp.float32)
    normed = modulated(running, modulation, 6)
    projected = jnp.einsum(
        "bfpd,de->bfpe",
        lax.all_gather(normed, "tp", axis=2, tiled=True),
        fc_in,
        preferred_element_type=jnp.float32,
    )
    hidden = jax.nn.gelu(projected, approximate=True).astype(jnp.bfloat16)
    partial_value = jnp.einsum("bfpe,ed->bfpd", hidden, fc_out, preferred_element_type=jnp.float32)
    mlp_out = lax.psum_scatter(
        partial_value.astype(jnp.bfloat16), "tp", scatter_dimension=2, tiled=True
    )
    return (running + modulation[:, 8][:, None, None, :] * mlp_out.astype(jnp.float32)).astype(
        jnp.bfloat16
    )


def body(n, latent, modulation, qkv_s, gain_s, out_s, qkv_t, gain_t, out_t, fc_in, fc_out):
    batches, frames, patches, width = latent.shape
    local = qkv_s.shape[-1]
    small = patches // n
    vmem = pl.BlockSpec(memory_space=pltpu.VMEM)
    hbm = pl.BlockSpec(memory_space=pl.ANY)
    dma = pltpu.SemaphoreType.DMA
    weights = (jnp.swapaxes(qkv_s, 1, 2), out_s, jnp.swapaxes(qkv_t, 1, 2), out_t, fc_in, fc_out)
    half = (batches, patches, width)
    blocks = (n, batches, small, width)
    pair = 1 + 4 * batches
    out = pl.pallas_call(
        functools.partial(kernel, n),
        out_shape=jax.ShapeDtypeStruct(half, BF16),
        in_specs=[vmem] * 4 + [hbm] * 6,
        out_specs=vmem,
        scratch_shapes=[pltpu.VMEM(w.shape, w.dtype) for w in weights]
        + [
            pltpu.VMEM(half, BF16),
            pltpu.VMEM((batches, 2 * patches, width), BF16),
            pltpu.VMEM(half, BF16),
            pltpu.VMEM(half, BF16),
            pltpu.VMEM(half, BF16),
            pltpu.VMEM(half, F32),
            pltpu.VMEM(blocks, BF16),
            pltpu.VMEM((2,) + blocks, BF16),
            pltpu.VMEM(blocks, BF16),
            pltpu.VMEM(blocks, BF16),
            pltpu.VMEM(half, BF16),
            pltpu.VMEM(half, BF16),
            pltpu.VMEM((2 * patches, fc_in.shape[1]), BF16),
            pltpu.VMEM((2 * patches, local), F32),
            dma((6,)),
            dma((pair,)),
            dma((pair,)),
        ]
        + [dma((batches * n,))] * 6
        + [dma((2 * batches,))],
        compiler_params=pltpu.CompilerParams(
            collective_id=0, has_side_effects=True, vmem_limit_bytes=62 * 1024 * 1024
        ),
    )(latent.reshape(half), jnp.swapaxes(modulation, 0, 1), gain_s, gain_t, *weights)
    return out.reshape(latent.shape)


def solution(mesh):
    n = mesh.shape["seq"]
    placed = (
        P(None, "seq", "tp", None),
        P(),
        P(None, None, "tp"),
        P(),
        P("tp", None),
        P(None, None, "tp"),
        P(),
        P("tp", None),
        P(None, "tp"),
        P("tp", None),
    )
    return jax.shard_map(
        functools.partial(body, n) if mesh.shape["tp"] == 2 else body_any_width,
        mesh=mesh,
        in_specs=placed,
        out_specs=P(None, "seq", "tp", None),
        check_vma=False,
    )
```
